256 devices in a mesh: groups: 4 (over x, y), expert: 32 (over z), mp: 2 (over core).
Axes of the slice: x: 2, y: 2, z: 32, core: 2. Of those that a mesh axis runs over, the one named last changes fastest.
The devices are a block of a 4x8x32 slice.
Arguments:
- residual: bfloat16 [4096, 5120], P(('groups', 'expert'), 'mp'), parts along dimension 0, may hold values from -6 to 6
- norm_gain: bfloat16 [5120], P('mp'), may hold values from 0.099609375 to 1.8984375
- router_weight: bfloat16 [640, 128], replicated, may hold values from -0.25 to 0.25
- expert_ids: int32 [4096, 8, 2], P(('groups', 'expert')), parts along dimension 0, may hold values from 0 to 127, all different within a row; in each aligned block of 256 rows (0 to 255, 256 to 511, ..., all dimensions but the last counted through in order) at most 5 rows name the same one
- expert_in: bfloat16 [128, 640, 1280], P('expert', None, 'mp'), may hold values from -0.25 to 0.25
- expert_out: bfloat16 [128, 1280, 640], P('expert', 'mp'), may hold values from -0.15625 to 0.15625
- queries: bfloat16 [4096, 5120], P(('groups', 'expert'), 'mp'), parts along dimension 0, may hold values from -6 to 6
- new_keys: bfloat16 [4096, 1024], P(('groups', 'expert'), 'mp'), parts along dimension 0, may hold values from -6 to 6
- new_values: bfloat16 [4096, 1024], P(('groups', 'expert'), 'mp'), parts along dimension 0, may hold values from -6 to 6
- cache_keys: bfloat16 [4096, 128, 1024], P(('groups', 'expert'), None, 'mp'), parts along dimension 0, may hold values from -6 to 6
- cache_values: bfloat16 [4096, 128, 1024], P(('groups', 'expert'), None, 'mp'), parts along dimension 0, may hold values from -6 to 6
- lengths: int32 [4096], P(('groups', 'expert')), parts along dimension 0, may hold values from 1 to 128
Outputs:
- attention: bfloat16 [4096, 5120], P(('groups', 'expert'), 'mp'), parts along dimension 0
- mixed: bfloat16 [4096, 5120], P(('groups', 'expert'), 'mp'), parts along dimension 0
The draws below stay inside these ranges and needn't reach their ends.
There are 4 independent parts, one for each index of `groups`. The reference program is written for one: setup_inputs(seed, part) draws one part's arguments, and reference() takes and returns one part's arrays. A program takes and returns all parts, laid end to end along the dimension named above; an argument that names none is the same for every part. Nothing has to cross between parts.
Inputs may be any that keep to these rules, and one draw needn't show every extreme that they name: `expert_ids`: within the 8 sub-tokens of each aligned block of 32 tokens, no expert is named more than 5 times, a bound that some block reaches; the 2 experts of one sub-token differ.
All inputs are finite; a program needn't handle non-finite values.
Results may differ from the reference program's by a relative error of at most 0.006.
Values may be sent and summed in bfloat16 or wider, within the bound.
A program may use at most 128 MiB of HBM per device.

```python
import math
import jax
import jax.numpy as jnp
import numpy as np
from jax import lax

D = 5120
SUB = 8
HEADS = 40
HD = 128
KV_HEADS = 8
EFF = 1280
EXPERTS = 128
TOP = 2
CAP = 5
CACHE = 128
TOK_DEV = 32
TOKENS = 1024
N_EXPERT = 32


def drawn_draw(key):
    base_key = jax.random.fold_in(key, 7001)
    subkeys = jax.random.split(base_key, 3)
    per_group = HEADS // KV_HEADS
    query_part = jnp.clip(jax.random.normal(subkeys[0], (TOKENS, KV_HEADS, per_group, HD), jnp.float32), -6.0, 6.0)
    cache_part = jnp.clip(jax.random.normal(subkeys[1], (TOKENS, CACHE, KV_HEADS, HD), jnp.float32), -6.0, 6.0)
    fresh_part = jnp.clip(jax.random.normal(subkeys[2], (TOKENS, KV_HEADS, HD), jnp.float32), -6.0, 6.0)
    return (query_part, cache_part, fresh_part)


def draw_queries(key, part):
    query_part, cache_part, fresh_part = drawn_draw(key)
    return query_part.reshape(TOKENS, HEADS * HD).astype(jnp.bfloat16)


def draw_cache_keys(key, part):
    query_part, cache_part, fresh_part = drawn_draw(key)
    return cache_part.reshape(TOKENS, CACHE, KV_HEADS * HD).astype(jnp.bfloat16)


def draw_new_keys(key, part):
    query_part, cache_part, fresh_part = drawn_draw(key)
    return fresh_part.reshape(TOKENS, KV_HEADS * HD).astype(jnp.bfloat16)


def with_ends(result, stream_key, low, high):
    shape = result.shape
    place = [jax.random.randint(jax.random.fold_in(stream_key, axis), (), 0, shape[axis]) for axis in range(len(shape))]
    result = result.at[tuple(place)].set(low)
    longest = shape.index(max(shape))
    place[longest] = (place[longest] + 1) % shape[longest]
    return result.at[tuple(place)].set(high)


def shard_levels(key, dims, cuts, least, top_value):
    level = 1.0
    for position, shards_of in cuts:
        heights = jax.random.uniform(jax.random.fold_in(jax.random.fold_in(key, 6), position), (shards_of,), jnp.float32, least / len(cuts), top_value / len(cuts))
        level = level * jnp.repeat(jnp.exp(heights), dims[position] // shards_of).reshape((-1,) + (1,) * (len(dims) - 1 - position))
    return level


def assign_block(rng, own, number, rows, count, top, limit, slope):
    ranking = jax.random.permutation(rng, count)
    heavy_load, common = load_shares(count, rows * top, limit, slope, True), load_shares(count, rows * top, limit, slope, False)
    places = jnp.arange(count)

    def named(sizes, rotation):
        used = int((sizes > 0).sum())
        fixed = max(1, used // 4)
        shifted = fixed + (places - fixed + rotation * (used - fixed)) % max(1, count - fixed)
        return jnp.zeros((count,), jnp.int32).at[ranking[jnp.where(places < fixed, places, shifted)]].set(jnp.asarray(sizes, jnp.int32))

    sizes = jnp.where(number % 4 == 0, named(heavy_load, number // 4), named(common, number - number // 4 - 1))
    mixed = jax.random.permutation(jax.random.fold_in(own, 3), count)
    giver, sink = mixed[0:count // 2 * 2:2], mixed[1:count // 2 * 2:2]
    room = jnp.minimum(sizes[giver] - 1, limit - sizes[sink]) // 2
    room = jnp.where((giver == ranking[0]) | (sink == ranking[0]) | (sizes[sink] == 0), 0, jnp.maximum(room, 0))
    shifted = jax.random.randint(jax.random.fold_in(own, 4), (count // 2,), 0, 1 << 20) % (room + 1)
    sizes = sizes.at[giver].add(-shifted).at[sink].add(shifted)
    labels = jnp.searchsorted(jnp.cumsum(sizes), jnp.arange(rows * top), side="right").astype(jnp.int32)
    grid = labels.reshape(top, rows).T
    grid = grid[jax.random.permutation(jax.random.fold_in(own, 1), rows)]
    rotation = jax.random.randint(jax.random.fold_in(own, 2), (rows, 1), 0, top)
    return jnp.take_along_axis(grid, (jnp.arange(top)[None, :] + rotation) % top, axis=1)


def load_shares(number_of, total, reach, slope, full):
    loads = [(1 << 20) // math.isqrt(grade ** slope) + 1 for grade in range(1, number_of + 1)]
    largest = reach if full else min(reach, max(-(-total // number_of), total * loads[0] // sum(loads)))
    least = 1 if total - largest >= number_of - 1 else 0
    holding, rest = [largest] + [least] * (number_of - 1), total - largest - least * (number_of - 1)
    while rest > 0:
        free = [i for i in range(1, number_of) if holding[i] < largest] or [i for i in range(1, number_of) if holding[i] < reach]
        whole, left = sum([loads[i] for i in free]), rest
        for i in free:
            extra = min(reach - holding[i], max(1, left * loads[i] // whole), rest)
            holding[i] = holding[i] + extra
            rest = rest - extra
    return np.array(holding)


def bell_draw(own_key, shape, spread, most, cuts=(), kind=jnp.bfloat16):
    array = jax.random.normal(own_key, shape, jnp.float32) * spread
    if len(cuts) > 0:
        array = shard_levels(own_key, shape, cuts, -0.22, 0.18) * array
    return jnp.clip(array, min=-most, max=most).astype(kind)


def setup_inputs(seed: int = 0, part: int = 0) -> dict:
    seeds = jax.random.split(jax.random.key(seed), 13)
    part_splits = jax.random.split(jax.random.fold_in(seeds[12], part), 13)
    residual = bell_draw(part_splits[0], (TOKENS, D), 1.0, 6.0, ((0, 32), (1, 2)))
    norm_gain = jnp.clip(1.0 + 0.18 * jax.random.normal(seeds[1], (D,), jnp.float32), 0.099609375, 1.8984375).astype(jnp.bfloat16)
    router_weight = bell_draw(seeds[2], (D // SUB, EXPERTS), (D // SUB) ** -0.5, 0.25)
    expert_ids_keys = jax.random.split(jax.random.fold_in(part_splits[3], 1), TOKENS * SUB // (TOK_DEV * SUB))
    expert_ids_turns = jax.random.permutation(jax.random.fold_in(part_splits[3], 3), TOKENS * SUB // (TOK_DEV * SUB))
    expert_ids = jax.vmap(lambda own, number: assign_block(jax.random.fold_in(part_splits[3], 2), own, number, TOK_DEV * SUB, EXPERTS, TOP, CAP, 2))(expert_ids_keys, expert_ids_turns).reshape((TOKENS, SUB, TOP))
    expert_in = bell_draw(seeds[4], (EXPERTS, D // SUB, EFF), (D // SUB) ** -0.5, 0.25, ((0, 32), (2, 2)))
    expert_out = bell_draw(seeds[5], (EXPERTS, EFF, D // SUB), EFF ** -0.5, 0.15625, ((0, 32), (1, 2)))
    queries = draw_queries(jax.random.fold_in(jax.random.fold_in(seeds[12], part), 71), part)
    new_keys = draw_new_keys(jax.random.fold_in(jax.random.fold_in(seeds[12], part), 71), part)
    new_values = bell_draw(part_splits[8], (TOKENS, KV_HEADS * HD), 1.0, 6.0, ((0, 32), (1, 2)))
    cache_keys = draw_cache_keys(jax.random.fold_in(jax.random.fold_in(seeds[12], part), 71), part)
    cache_values = bell_draw(part_splits[10], (TOKENS, CACHE, KV_HEADS * HD), 1.0, 6.0, ((0, 32), (2, 2)))
    lengths = with_ends(jax.random.randint(part_splits[11], (TOKENS,), 1, CACHE + 1), jax.random.fold_in(part_splits[11], 1), 1, CACHE).astype(jnp.int32)
    return {"residual": residual, "norm_gain": norm_gain, "router_weight": router_weight, "expert_ids": expert_ids, "expert_in": expert_in, "expert_out": expert_out, "queries": queries, "new_keys": new_keys, "new_values": new_values, "cache_keys": cache_keys, "cache_values": cache_values, "lengths": lengths}


def normalize(residual, norm_gain):
    sub_width = D // SUB
    pieces = residual.astype(jnp.float32).reshape(residual.shape[0], -1, sub_width)
    gain_rows = norm_gain.astype(jnp.float32).reshape(-1, sub_width)
    meansq = lax.optimization_barrier(jnp.mean(pieces * pieces, axis=-1, keepdims=True))
    return (pieces * lax.rsqrt(meansq + 1e-06) * gain_rows).astype(jnp.bfloat16)

def route_weights(normed, router_weight, chosen_ids):
    logits = jnp.einsum('tsw,we->tse', normed.astype(jnp.float32), router_weight.astype(jnp.float32))
    onehot = (chosen_ids[..., None] == jnp.arange(EXPERTS, dtype=jnp.int32)).astype(jnp.float32)
    picked = lax.optimization_barrier(jnp.sum(onehot * logits[:, :, None, :], axis=-1))
    scores = jax.nn.sigmoid(picked)
    return scores / lax.optimization_barrier(jnp.sum(scores, axis=-1, keepdims=True))

def attend(queries, new_keys, new_values, cache_keys, cache_values, lengths):
    tokens = queries.shape[0]
    groups = KV_HEADS
    per_group = HEADS // KV_HEADS
    score_scale = 1.0 / math.sqrt(HD)
    query_heads = queries.astype(jnp.float32).reshape(tokens, groups, per_group, HD)
    keys_old = cache_keys.astype(jnp.float32).reshape(tokens, CACHE, groups, HD)
    values_old = cache_values.astype(jnp.float32).reshape(tokens, CACHE, groups, HD)
    keys_new = new_keys.astype(jnp.float32).reshape(tokens, groups, HD)
    values_new = new_values.astype(jnp.float32).reshape(tokens, groups, HD)
    scores = jnp.einsum('tgqd,tjgd->tgqj', query_heads, keys_old) * score_scale
    fresh_score = jnp.einsum('tgqd,tgd->tgq', query_heads, keys_new) * score_scale
    usable = (jnp.arange(CACHE, dtype=jnp.int32)[None, :] < lengths[:, None])[:, None, None, :]
    scores = jnp.where(usable, scores, -1e+30)
    row_max = jnp.maximum(lax.optimization_barrier(jnp.max(scores, axis=-1)), fresh_score)
    expo_old = jnp.where(usable, jnp.exp(scores - row_max[..., None]), 0.0)
    expo_new = jnp.exp(fresh_score - row_max)
    totals = lax.optimization_barrier(jnp.sum(expo_old, axis=-1)) + expo_new
    cache_probs = (expo_old / totals[..., None]).astype(jnp.bfloat16)
    fresh_probs = (expo_new / totals).astype(jnp.bfloat16)
    context = jnp.einsum('tgqj,tjgd->tgqd', cache_probs.astype(jnp.float32), values_old)
    context = context + fresh_probs.astype(jnp.float32)[..., None] * values_new[:, :, None, :]
    return context.reshape(tokens, D)

def reference(residual, norm_gain, router_weight, expert_ids, expert_in, expert_out, queries, new_keys, new_values, cache_keys, cache_values, lengths):
    sub_width = D // SUB
    normed = normalize(residual, norm_gain)
    weights = route_weights(normed, router_weight, expert_ids)
    flat_ids = expert_ids.reshape(-1).astype(jnp.int32)
    onehot = (flat_ids[:, None] == jnp.arange(EXPERTS, dtype=jnp.int32)[None, :]).astype(jnp.int32)
    before = jnp.cumsum(onehot, axis=0) - onehot
    slot_index = lax.optimization_barrier(jnp.sum(before * onehot, axis=1)).astype(jnp.int32)
    depth = N_EXPERT * CAP
    target = (flat_ids * depth + slot_index).astype(jnp.int32)
    sources = jnp.broadcast_to(normed[:, :, None, :], (TOKENS, SUB, TOP, sub_width)).reshape(-1, sub_width)
    buffer = jnp.zeros((EXPERTS * depth, sub_width), jnp.bfloat16).at[target].set(sources)
    buffer = buffer.reshape(EXPERTS, depth, sub_width)
    hidden = jax.nn.gelu(jnp.einsum('emw,ewf->emf', buffer.astype(jnp.float32), expert_in.astype(jnp.float32))).astype(jnp.bfloat16)
    output = jnp.einsum('emf,efw->emw', hidden.astype(jnp.float32), expert_out.astype(jnp.float32)).astype(jnp.bfloat16)
    picked = output.reshape(EXPERTS * depth, sub_width)[target].astype(jnp.float32)
    picked = picked.reshape(TOKENS, SUB, TOP, sub_width)
    moe = lax.optimization_barrier(jnp.sum(weights[..., None] * picked, axis=2)).reshape(TOKENS, D)
    context = attend(queries, new_keys, new_values, cache_keys, cache_values, lengths)
    attention = context.astype(jnp.bfloat16)
    mixed = (residual.astype(jnp.float32) + context + moe).astype(jnp.bfloat16)
    return (attention, mixed)
```

```python
import functools
import math

import jax
import jax.numpy as jnp
from jax import lax
from jax.experimental import pallas as pl
from jax.experimental.pallas import tpu as pltpu
from jax.sharding import PartitionSpec as P

MESH = pl.DeviceIdType.MESH
F32 = jnp.float32
BF16 = jnp.bfloat16

SUB = 8
TOP = 2
CAP = 5
HD = 128
PER_GROUP = 5
CHUNK = 4
TOKEN_BLOCK = 8


def dot(a, b, dims=((1,), (0,))):
    return lax.dot_general(a, b, (dims, ((), ())), preferred_element_type=F32)


def gelu(v):
    return 0.5 * v * (1.0 + jnp.tanh(math.sqrt(2.0 / math.pi) * (v + 0.044715 * (v * v * v))))


def place(ring, delta):
    away = jnp.minimum(delta, ring - delta)
    behind = jnp.where(delta > ring // 2, 1, 0)
    return jnp.maximum(ring - 1 - 2 * away + behind, 0)


def delta_at(ring, pos):
    away = (ring - pos) // 2
    behind = jnp.where((pos % 2 == 0) & (pos > 0), 1, 0)
    return (ring + away - 2 * away * behind) % ring


def kernel(
    ring,
    res_ref,
    gain_ref,
    router_ref,
    ids_row_ref,
    ids_col_ref,
    query_ref,
    new_key_ref,
    new_value_ref,
    lengths_ref,
    w_in_ref,
    w_out_ref,
    keys_ref,
    values_ref,
    ctx_ref,
    moe_ref,
    normed,
    outbuf,
    inbuf,
    resbuf,
    retbuf,
    w_in,
    w_out,
    keys,
    values,
    acc,
    other,
    load_sem,
    pair_send,
    pair_recv,
    out_send,
    out_recv,
    ret_send,
    ret_recv,
):
    me = lax.axis_index("expert")
    core = lax.axis_index("mp")
    tokens, width = res_ref.shape
    sub_local = SUB // 2
    sub_width = width // sub_local
    own_rows = tokens * sub_local
    rows = 2 * own_rows
    experts = router_ref.shape[1]
    per_pair = 2 * CAP
    slots = ring * per_pair

    barrier = pltpu.get_barrier_semaphore()

    def greet(step, carry):
        pl.semaphore_signal(
            barrier, inc=1, device_id={"expert": (me + step) % ring}, device_id_type=MESH
        )
        return carry

    lax.fori_loop(1, ring, greet, 0)
    pl.semaphore_signal(barrier, inc=1, device_id={"mp": 1 - core}, device_id_type=MESH)

    loads = [
        pltpu.make_async_copy(w_in_ref.at[pl.ds(2 * core, 2)], w_in.at[0], load_sem.at[0]),
        pltpu.make_async_copy(w_out_ref.at[pl.ds(2 * core, 2)], w_out.at[0], load_sem.at[1]),
        pltpu.make_async_copy(keys_ref, keys, load_sem.at[2]),
        pltpu.make_async_copy(values_ref, values, load_sem.at[3]),
    ]
    for load in loads:
        load.start()

    for s in range(sub_local):
        cut = slice(s * sub_width, (s + 1) * sub_width)
        piece = res_ref[:, cut].astype(F32)
        meansq = jnp.mean(piece * piece, axis=-1, keepdims=True)
        scaled = piece * lax.rsqrt(meansq + 1e-06) * gain_ref[:, cut].astype(F32)
        normed[pl.ds(core * own_rows + s * tokens, tokens), :] = scaled.astype(BF16)

    def slot_of(ids, rank):
        delta = ((ids >> 2) - me + ring) % ring
        slot = place(ring, delta) * per_pair + rank.astype(jnp.int32) * 2 + (ids & 1)
        return jnp.where(((ids >> 1) & 1) == core, slot, -1)

    expert_rows = lax.broadcasted_iota(jnp.int32, (experts, rows), 0)
    named = [
        (expert_rows == ids_row_ref[k : k + 1, :]).astype(F32) for k in range(TOP)
    ]
    earlier = (
        lax.broadcasted_iota(jnp.int32, (rows, rows), 0)
        < lax.broadcasted_iota(jnp.int32, (rows, rows), 1)
    ).astype(BF16)
    before = dot((named[0] + named[1]).astype(BF16), earlier)
    slot_rows = lax.broadcasted_iota(jnp.int32, (slots, rows), 0)
    slot_row = [
        slot_of(ids_row_ref[k : k + 1, :], jnp.sum(named[k] * before, axis=0, keepdims=True))
        for k in range(TOP)
    ]
    dispatch = ((slot_rows == slot_row[0]) | (slot_rows == slot_row[1])).astype(BF16)

    pl.semaphore_wait(barrier, ring)

    def to_partner(src, dst, index):
        return pltpu.make_async_remote_copy(
            src_ref=src,
            dst_ref=dst,
            send_sem=pair_send.at[index],
            recv_sem=pair_recv.at[index],
            device_id={"mp": 1 - core},
            device_id_type=MESH,
        )

    mine = normed.at[pl.ds(core * own_rows, own_rows)]
    share = to_partner(mine, mine, 0)
    share.start()
    swaps = [
        to_partner(w_in_ref.at[pl.ds(2 * (1 - core), 2)], w_in.at[1], 1),
        to_partner(w_out_ref.at[pl.ds(2 * (1 - core), 2)], w_out.at[1], 2),
    ]
    for swap in swaps:
        swap.start()
    share.wait()

    outgoing = dot(dispatch, normed[...]).astype(BF16)
    outbuf[...] = outgoing.reshape(ring, CAP, 2, sub_width)
    inbuf[ring - 1] = outbuf[ring - 1]

    def outward(pos):
        return pltpu.make_async_remote_copy(
            src_ref=outbuf.at[pos],
            dst_ref=inbuf.at[pos],
            send_sem=out_send.at[pos],
            recv_sem=out_recv.at[pos],
            device_id={"expert": (me + delta_at(ring, pos)) % ring},
            device_id_type=MESH,
        )

    def homeward(pos):
        return pltpu.make_async_remote_copy(
            src_ref=resbuf.at[pos],
            dst_ref=retbuf.at[pos],
            send_sem=ret_send.at[pos],
            recv_sem=ret_recv.at[pos],
            device_id={"expert": (me + ring - delta_at(ring, pos)) % ring},
            device_id_type=MESH,
        )

    def send_out(pos, carry):
        outward(pos).start()
        return carry

    lax.fori_loop(0, ring - 1, send_out, 0)

    loads[2].wait()
    loads[3].wait()
    cache_len = keys.shape[1]
    kv_local = keys.shape[2] // HD
    score_scale = 1.0 / math.sqrt(HD)

    def attend(block, carry):
        contexts = []
        for b in range(TOKEN_BLOCK):
            context_of = []
            t = block * TOKEN_BLOCK + b
            scores, fresh = [], []
            for g in range(kv_local):
                cut = slice(g * HD, (g + 1) * HD)
                q = query_ref[t, g]
                scores.append(dot(q, keys[t, :, cut], ((1,), (1,))))
                key = new_key_ref[t, :, cut]
                fresh.append(jnp.sum(q.astype(F32) * key, axis=-1, keepdims=True))
            score = jnp.concatenate(scores, axis=0) * score_scale
            fresh_score = jnp.concatenate(fresh, axis=0) * score_scale
            usable = lax.broadcasted_iota(jnp.int32, score.shape, 1) < lengths_ref[t]
            score = jnp.where(usable, score, -1e30)
            row_max = jnp.maximum(jnp.max(score, axis=-1, keepdims=True), fresh_score)
            expo = jnp.where(usable, jnp.exp(score - row_max), 0.0)
            expo_new = jnp.exp(fresh_score - row_max)
            total = jnp.sum(expo, axis=-1, keepdims=True) + expo_new
            probs = (expo / total).astype(BF16)
            fresh_probs = (expo_new / total).astype(BF16).astype(F32)
            for g in range(kv_local):
                cut = slice(g * HD, (g + 1) * HD)
                part = slice(g * 8, (g + 1) * 8)
                context = dot(probs[part], values[t, :, cut])
                context_of.append(context + fresh_probs[part] * new_value_ref[t, :, cut])
            contexts.append(context_of)
        at = pl.ds(pl.multiple_of(block * TOKEN_BLOCK, TOKEN_BLOCK), TOKEN_BLOCK)
        for g in range(kv_local):
            for h in range(PER_GROUP):
                head = g * PER_GROUP + h
                lines = [context_of[g][h : h + 1] for context_of in contexts]
                ctx_ref[at, head * HD : (head + 1) * HD] = jnp.concatenate(lines, axis=0)
        return carry

    lax.fori_loop(0, tokens // TOKEN_BLOCK, attend, 0)

    loads[0].wait()
    loads[1].wait()
    for swap in swaps:
        swap.wait()

    even = lax.broadcasted_iota(jnp.int32, (CHUNK * per_pair, sub_width), 0) % 2 == 0

    def serve(chunk, carry):
        first = chunk * CHUNK
        for b in range(CHUNK):
            pos = first + b

            @pl.when(pos < ring - 1)
            def _():
                outward(pos).wait_recv()

        x = inbuf[pl.ds(first, CHUNK)].reshape(CHUNK * per_pair, sub_width)
        y = jnp.zeros((CHUNK * per_pair, sub_width), F32)
        for half in range(2):
            v = jnp.where(even, dot(x, w_in[half, 0]), dot(x, w_in[half, 1]))
            hidden = gelu(v).astype(BF16)
            none = jnp.zeros_like(hidden)
            y = y + dot(jnp.where(even, hidden, none), w_out[half, 0])
            y = y + dot(jnp.where(even, none, hidden), w_out[half, 1])
        resbuf[pl.ds(first, CHUNK)] = y.astype(BF16).reshape(CHUNK, CAP, 2, sub_width)
        for b in range(CHUNK):
            pos = first + b

            @pl.when(pos < ring - 1)
            def _():
                homeward(pos).start()

        return carry

    lax.fori_loop(0, ring // CHUNK, serve, 0)
    retbuf[ring - 1] = resbuf[ring - 1]

    expert_cols = lax.broadcasted_iota(jnp.int32, (rows, experts), 1)
    logits = dot(normed[...], router_ref[...])
    named = [(expert_cols == ids_col_ref[:, k : k + 1]).astype(F32) for k in range(TOP)]
    earlier = (
        lax.broadcasted_iota(jnp.int32, (rows, rows), 1)
        < lax.broadcasted_iota(jnp.int32, (rows, rows), 0)
    ).astype(BF16)
    before = dot(earlier, (named[0] + named[1]).astype(BF16))
    gate, slot_col = [], []
    for k in range(TOP):
        picked = jnp.sum(named[k] * logits, axis=-1, keepdims=True)
        gate.append(1.0 / (1.0 + jnp.exp(-picked)))
        rank = jnp.sum(named[k] * before, axis=-1, keepdims=True)
        slot_col.append(slot_of(ids_col_ref[:, k : k + 1], rank))
    gate_sum = gate[0] + gate[1]
    weight = [g / gate_sum for g in gate]

    groups = 4
    span = ring // groups
    for group in range(groups):
        first = group * span
        for pos in range(first, min(first + span, ring - 1)):
            homeward(pos).wait_recv()
        back = retbuf[first : first + span].reshape(span * per_pair, sub_width)
        cols = lax.broadcasted_iota(jnp.int32, (rows, span * per_pair), 1) + first * per_pair
        part = weight[0] * dot((cols == slot_col[0]).astype(BF16), back)
        part = part + weight[1] * dot((cols == slot_col[1]).astype(BF16), back)
        acc[...] = part if group == 0 else acc[...] + part

    hand = to_partner(acc.at[pl.ds((1 - core) * own_rows, own_rows)], other, 3)
    hand.start()

    def sent(pos, carry):
        outward(pos).wait_send()
        homeward(pos).wait_send()
        return carry

    lax.fori_loop(0, ring - 1, sent, 0)
    hand.wait()
    for s in range(sub_local):
        cut = slice(s * sub_width, (s + 1) * sub_width)
        own = acc[pl.ds(core * own_rows + s * tokens, tokens), :]
        moe_ref[:, cut] = own + other[s * tokens : (s + 1) * tokens, :]


def solution(mesh):
    ring = mesh.shape["expert"]

    def per_device(
        residual,
        norm_gain,
        router_weight,
        expert_ids,
        expert_in,
        expert_out,
        queries,
        new_keys,
        new_values,
        cache_keys,
        cache_values,
        lengths,
    ):
        tokens, width = residual.shape
        sub_width = router_weight.shape[0]
        rows = tokens * SUB
        kv_local = new_keys.shape[1] // HD
        half_hidden = expert_in.shape[2]
        ids_row = expert_ids.transpose(2, 1, 0).reshape(TOP, rows)
        ids_col = expert_ids.transpose(1, 0, 2).reshape(rows, TOP)
        query = jnp.pad(
            queries.reshape(tokens, kv_local, PER_GROUP, HD),
            ((0, 0), (0, 0), (0, 8 - PER_GROUP), (0, 0)),
        )
        vmem = pl.BlockSpec(memory_space=pltpu.VMEM)
        hbm = pl.BlockSpec(memory_space=pl.ANY)
        smem = pl.BlockSpec(memory_space=pltpu.SMEM)
        block = (ring, CAP, 2, sub_width)
        context, moe = pl.pallas_call(
            functools.partial(kernel, ring),
            out_shape=[jax.ShapeDtypeStruct((tokens, width), F32)] * 2,
            in_specs=[vmem] * 8 + [smem] + [hbm] * 4,
            out_specs=[vmem] * 2,
            scratch_shapes=[
                pltpu.VMEM((rows, sub_width), BF16),
                pltpu.VMEM(block, BF16),
                pltpu.VMEM(block, BF16),
                pltpu.VMEM(block, BF16),
                pltpu.VMEM(block, BF16),
                pltpu.VMEM((2, 2, sub_width, half_hidden), BF16),
                pltpu.VMEM((2, 2, half_hidden, sub_width), BF16),
                pltpu.VMEM(cache_keys.shape, BF16),
                pltpu.VMEM(cache_values.shape, BF16),
                pltpu.VMEM((rows, sub_width), F32),
                pltpu.VMEM((rows // 2, sub_width), F32),
                pltpu.SemaphoreType.DMA((4,)),
                pltpu.SemaphoreType.DMA((4,)),
                pltpu.SemaphoreType.DMA((4,)),
                pltpu.SemaphoreType.DMA((ring,)),
                pltpu.SemaphoreType.DMA((ring,)),
                pltpu.SemaphoreType.DMA((ring,)),
                pltpu.SemaphoreType.DMA((ring,)),
            ],
            compiler_params=pltpu.CompilerParams(collective_id=0, has_side_effects=True),
            name="step",
        )(
            residual,
            norm_gain.reshape(1, width),
            router_weight,
            ids_row,
            ids_col,
            query,
            new_keys.astype(F32).reshape(tokens, 1, -1),
            new_values.astype(F32).reshape(tokens, 1, -1),
            lengths,
            expert_in,
            expert_out,
            cache_keys,
            cache_values,
        )
        attention = context.astype(BF16)
        mixed = (residual.astype(F32) + context + moe).astype(BF16)
        return attention, mixed

    both = ("groups", "expert")
    placed = (
        P(both, "mp"),
        P("mp"),
        P(),
        P(both, None, None),
        P("expert", None, "mp"),
        P("expert", "mp", None),
        P(both, "mp"),
        P(both, "mp"),
        P(both, "mp"),
        P(both, None, "mp"),
        P(both, None, "mp"),
        P(both),
    )
    return jax.shard_map(
        per_device,
        mesh=mesh,
        in_specs=placed,
        out_specs=(P(both, "mp"), P(both, "mp")),
        check_vma=False,
    )
```
